32 devices in a mesh: seq: 16 (over z, x, core), chan: 2 (over y).
Axes of the slice: x: 2, y: 2, z: 4, core: 2. Of those that a mesh axis runs over, the one named last changes fastest.
Arguments:
- step_size: bfloat16 [2, 5120, 2048], P(None, ('chan', 'seq')), as said below
- inputs: bfloat16 [2, 5120, 2048], P(None, ('chan', 'seq')), may hold values from -6 to 6
- gate_input: bfloat16 [2, 5120, 2048], P(None, ('chan', 'seq')), may hold values from -6 to 6
- decay_rate: float32 [5120], P('chan'), as said below
- norm_gain: float32 [5120], P('chan'), may hold values from 0.1 to 1.9
- resets: int32 [2, 8], replicated, may hold values from 1 to 2047
Outputs:
- normed: bfloat16 [2, 5120, 2048], P(None, 'chan', 'seq')
The draws below stay inside these ranges and needn't reach their ends.
Inputs may be any that keep to these rules, and one draw needn't show every extreme that they name: `step_size`: positive step sizes. `decay_rate`: positive rates. `resets`: positions within the sequence; several may coincide.
All inputs are finite; a program needn't handle non-finite values.
Results may differ from the reference program's by a relative error of at most 0.001.
Values may be sent and summed in bfloat16 or wider, within the bound.
A program may use at most 64 MiB of HBM per device.

```python
import math
import jax
import jax.numpy as jnp
from jax import lax

FEATURE_WIDTH = 5120
BATCH_SIZE = 2
NDOC = 8
TOKENS_PER_ROW = 2048


def draw_step_size(key, part):
    first, second, final_segment = jax.random.split(key, 3)
    starting_index = jnp.exp(jax.random.uniform(first, (BATCH_SIZE, FEATURE_WIDTH, TOKENS_PER_ROW), jnp.float32, math.log(0.5), math.log(2.0)))
    places = jax.random.randint(second, (BATCH_SIZE, 4), 0, TOKENS_PER_ROW)
    restart_flags = jnp.any(places[:, :, None] == jnp.arange(TOKENS_PER_ROW)[None, None, :], axis=1)
    restart_runs = 0.35 * TOKENS_PER_ROW * jax.random.uniform(final_segment, (BATCH_SIZE, FEATURE_WIDTH, TOKENS_PER_ROW), jnp.float32, 0.7, 1.4)
    return jnp.where(restart_flags[:, None, :], restart_runs, starting_index).astype(jnp.bfloat16)


def draw_decay_rate(key, part):
    first, second, final_segment = jax.random.split(key, 3)
    slow = jnp.exp(jax.random.uniform(first, (FEATURE_WIDTH,), jnp.float32, math.log(0.5 / TOKENS_PER_ROW), math.log(2.0 / TOKENS_PER_ROW)))
    quick = jnp.exp(jax.random.uniform(second, (FEATURE_WIDTH,), jnp.float32, math.log(2.0 / TOKENS_PER_ROW), math.log(0.05)))
    share = 0.5
    picks = jax.random.uniform(final_segment, (FEATURE_WIDTH,), jnp.float32) < share
    return jnp.where(picks, slow, quick).astype(jnp.float32)


def touch_ends(drawn, own_key, low, largest):
    shape = drawn.shape
    index_at = [jax.random.randint(jax.random.fold_in(own_key, axis), (), 0, shape[axis]) for axis in range(len(shape))]
    drawn = drawn.at[tuple(index_at)].set(low)
    longest = shape.index(max(shape))
    index_at[longest] = (index_at[longest] + 1) % shape[longest]
    return drawn.at[tuple(index_at)].set(largest)


def steps_of(key, shape, cuts, least, high):
    gain, own = 1.0, jax.random.fold_in(key, 6)
    for axis_at, shards_of in cuts:
        steps = jnp.exp(jax.random.uniform(jax.random.fold_in(own, axis_at), (shards_of,), jnp.float32, least / len(cuts), high / len(cuts)))
        gain = gain * jnp.repeat(steps, shape[axis_at] // shards_of).reshape([-1 if axis == axis_at else 1 for axis in range(len(shape))])
    return gain


def bell_draw(rng, dims, scale, most, cuts=(), held_as=jnp.bfloat16):
    values = scale * jax.random.normal(rng, dims, jnp.float32)
    if cuts:
        values = values * steps_of(rng, dims, cuts, -0.22, 0.18)
    return jnp.clip(values, -most, most).astype(held_as)


def setup_inputs(seed: int = 0) -> dict:
    key_list = jax.random.split(jax.random.key(seed), 7)
    return {
        "step_size": draw_step_size(jax.random.fold_in(key_list[6], 71), 0),
        "inputs": bell_draw(key_list[1], (BATCH_SIZE, FEATURE_WIDTH, TOKENS_PER_ROW), 1.0, 6.0, ((1, 32),)),
        "gate_input": bell_draw(key_list[2], (BATCH_SIZE, FEATURE_WIDTH, TOKENS_PER_ROW), 1.0, 6.0, ((1, 32),)),
        "decay_rate": draw_decay_rate(jax.random.fold_in(key_list[6], 71), 0),
        "norm_gain": jnp.clip(1.0 + 0.18 * jax.random.normal(key_list[4], (FEATURE_WIDTH,), jnp.float32), 0.1, 1.9),
        "resets": touch_ends(jax.random.randint(key_list[5], (BATCH_SIZE, NDOC), 1, TOKENS_PER_ROW), jax.random.fold_in(key_list[5], 1), 1, TOKENS_PER_ROW - 1).astype(jnp.int32),
    }


def reference(step_size, inputs, gate_input, decay_rate, norm_gain, resets):
    length = step_size.shape[2]
    places = jnp.arange(length, dtype=jnp.int32)
    reset_mask = jnp.any(resets[:, :, None] == places[None, None, :], axis=1)

    def advance(state, pieces):
        steps, values, marks = pieces
        scaled = steps.astype(jnp.float32) * decay_rate[None, :]
        decay = jnp.where(marks[:, None], jnp.float32(0.0), jnp.exp(-scaled))
        drive = jnp.sqrt(-jnp.expm1(-2.0 * scaled)) * values.astype(jnp.float32)
        state = decay * state + drive
        return (state, state)
    start = jnp.zeros((step_size.shape[0], step_size.shape[1]), jnp.float32)
    _, states = lax.scan(advance, start, (jnp.moveaxis(step_size, 2, 0), jnp.moveaxis(inputs, 2, 0), reset_mask.T))
    state = jnp.moveaxis(states, 0, 2)
    gated = state * jax.nn.silu(gate_input.astype(jnp.float32))
    mean_square = lax.optimization_barrier(jnp.mean(gated * gated, axis=1, keepdims=True))
    return (gated * lax.rsqrt(mean_square + 1e-05) * norm_gain[None, :, None]).astype(jnp.bfloat16)
```

```python
import functools
import math

import jax
import jax.numpy as jnp
from jax import lax
from jax.experimental import pallas as pl
from jax.experimental.pallas import tpu as pltpu
from jax.sharding import PartitionSpec as P

FEATURE_WIDTH = 5120


def compose(earlier, later):
    return (earlier[0] * later[0], later[0] * earlier[1] + later[1])


def coefficients(steps, values, rates):
    scaled = steps.astype(jnp.float32) * rates[None, :, None]
    drive = jnp.sqrt(-jnp.expm1(-2.0 * scaled)) * values.astype(jnp.float32)
    return (scaled, drive)


def marks_for(resets, places):
    return jnp.any(resets[:, :, None] == places[None, None, :], axis=1)


def local_scan(scaled, drive, marks):
    rows, chans, length = scaled.shape
    places = jnp.arange(length, dtype=jnp.int32)
    upper = (places[:, None] <= places[None, :]).astype(jnp.float32)
    cumul = jnp.einsum("rck,ku->rcu", scaled, upper, precision=lax.Precision.HIGHEST)
    counts = jnp.dot(marks.astype(jnp.float32), upper, precision=lax.Precision.HIGHEST)
    linked = (counts[:, :, None] == counts[:, None, :]) & (places[:, None] >= places[None, :])[None]
    group = math.gcd(chans, 64)

    def one_group(pieces):
        cumul_part, drive_part = pieces
        spread = cumul_part[:, :, :, None] - cumul_part[:, :, None, :]
        weight = jnp.where(linked[:, None], jnp.exp(-jnp.maximum(spread, 0.0)), jnp.float32(0.0))
        return jnp.einsum("rctj,rcj->rct", weight, drive_part, precision=lax.Precision.HIGHEST)

    def split_groups(array):
        return jnp.moveaxis(array.reshape(rows, chans // group, group, length), 1, 0)

    results = lax.map(one_group, (split_groups(cumul), split_groups(drive)))
    local_state = jnp.moveaxis(results, 0, 1).reshape(rows, chans, length)
    running = jnp.where(counts[:, None, :] == 0.0, jnp.exp(-cumul), jnp.float32(0.0))
    return (running, local_state)


def finish(gated, norm_gain):
    squares = jnp.sum(gated * gated, axis=1)
    total = lax.psum(squares, "chan")
    mean_square = total / jnp.float32(FEATURE_WIDTH)
    scale_rows = lax.rsqrt(mean_square + 1e-05)
    return (gated * scale_rows[:, None, :] * norm_gain[None, :, None]).astype(jnp.bfloat16)


def per_device(step_size, inputs, gate_input, decay_rate, norm_gain, resets):
    position = lax.axis_index("seq")
    batch, width, length = step_size.shape
    rates = lax.dynamic_slice_in_dim(decay_rate, position * width, width)
    places = jnp.arange(length, dtype=jnp.int32)
    scaled, drive = coefficients(step_size, inputs, rates)
    marks = marks_for(resets, places)
    piece = math.gcd(length, 128)
    count_blocks = length // piece

    def to_blocks(array):
        moved = jnp.moveaxis(array.reshape(batch, width, count_blocks, piece), 2, 1)
        return moved.reshape(batch * count_blocks, width, piece)

    running, local_state = local_scan(
        to_blocks(scaled), to_blocks(drive), marks.reshape(batch * count_blocks, piece)
    )
    total_decay = running[:, :, -1].reshape(batch, count_blocks, width)
    total_state = local_state[:, :, -1].reshape(batch, count_blocks, width)
    prefix = lax.associative_scan(compose, (total_decay, total_state), axis=1)
    incoming = jnp.concatenate(
        [jnp.zeros((batch, 1, width), jnp.float32), prefix[1][:, :-1]], axis=1
    )
    blocked = local_state + running * incoming.reshape(batch * count_blocks, width)[:, :, None]
    state = jnp.moveaxis(blocked.reshape(batch, count_blocks, width, piece), 1, 2).reshape(
        batch, width, length
    )
    local_gated = state * jax.nn.silu(gate_input.astype(jnp.float32))
    gated = lax.all_to_all(local_gated, "seq", split_axis=2, concat_axis=1, tiled=True)
    return finish(gated, norm_gain)


LANES = 128
ROWS = 16
UNROLL = 4
MESH = pl.DeviceIdType.MESH


def scan_blocks(pairs, lane):
    shift = 1
    while shift < LANES:
        inside = lane >= shift
        advanced = []
        for decay, drive in pairs:
            masked = jnp.where(inside, decay, 0.0)
            drive = drive + masked * pltpu.roll(drive, shift, 1)
            decay = jnp.where(inside, decay * pltpu.roll(decay, shift, 1), decay)
            advanced.append((decay, drive))
        pairs = advanced
        shift *= 2
    return pairs


def kernel(
    seq_size, chan_size, resets_ref, step_ref, in_ref, gate_ref, rate_ref, gain_ref, out_ref,
    step_v, in_v, gate_v, gated, send_v, keep, squares, sums, parts, scales,
    load_sem, part_send, part_recv, scale_send, scale_recv, data_send, data_recv, own_sem,
):
    batch, width, length = step_v.shape
    blocks = length // LANES
    devices = seq_size * chan_size
    my_seq, my_chan = lax.axis_index("seq"), lax.axis_index("chan")
    mine = my_seq * chan_size + my_chan

    loads = []
    for b in range(batch):
        group = []
        for i, (src, dst) in enumerate(((step_ref, step_v), (in_ref, in_v), (gate_ref, gate_v))):
            group.append(pltpu.make_async_copy(src.at[b], dst.at[b], load_sem.at[b, i]))
        for copy in group:
            copy.start()
        loads.append(group)

    def peer(d):
        other = lax.rem(mine + d, devices)
        return other // chan_size, lax.rem(other, chan_size), other

    barrier = pltpu.get_barrier_semaphore()

    @pl.loop(1, devices)
    def _(d):
        ps, pc, _ = peer(d)
        pl.semaphore_signal(barrier, inc=1, device_id=(ps, pc), device_id_type=MESH)

    lane = lax.broadcasted_iota(jnp.int32, (ROWS, LANES), 1)
    lane_row = lax.broadcasted_iota(jnp.int32, (8, LANES), 1)
    zero_rows = jnp.zeros((8, LANES), jnp.float32)

    def prepare(b):
        @pl.loop(0, blocks)
        def _(t):
            place = lane_row + t * LANES
            hit = place == resets_ref[b, 0]
            for k in range(1, resets_ref.shape[1]):
                hit = hit | (place == resets_ref[b, k])
            keep[t] = jnp.where(hit, 0.0, 1.0)
            squares[b, t] = zero_rows

    def compute(b, first, last):
        @pl.loop(first, last)
        def _(r):
            rows = pl.ds(pl.multiple_of(r * ROWS, ROWS), ROWS)
            rate = rate_ref[rows, :]

            def step(sup, carry):
                pairs, silus = [], []
                for u in range(UNROLL):
                    t = sup * UNROLL + u
                    lanes = pl.ds(pl.multiple_of(t * LANES, LANES), LANES)
                    x = step_v[b, rows, lanes].astype(jnp.float32) * rate
                    a = jnp.exp(-x)
                    y = x + x
                    series = y * (1.0 - y * (1 / 2 - y * (1 / 6 - y * (1 / 24 - y * (1 / 120 - y * (1 / 720))))))
                    z = jnp.where(y < 0.25, series, 1.0 - a * a)
                    root = z * lax.rsqrt(jnp.maximum(z, 1e-37))
                    drive = root * in_v[b, rows, lanes].astype(jnp.float32)
                    k8 = keep[t]
                    decay = a * jnp.concatenate([k8] * (ROWS // 8), axis=0)
                    pairs.append((decay, drive))
                pairs = scan_blocks(pairs, lane)
                for u in range(UNROLL):
                    t = sup * UNROLL + u
                    lanes = pl.ds(pl.multiple_of(t * LANES, LANES), LANES)
                    decay, drive = pairs[u]
                    state = drive + decay * carry
                    carry = jnp.broadcast_to(state[:, LANES - 1 :], (ROWS, LANES))
                    v = gate_v[b, rows, lanes].astype(jnp.float32)
                    g = state * (v / (1.0 + jnp.exp(-v)))
                    gated[b, t, rows, :] = g
                    sq = g * g
                    part = sq[:8]
                    for i in range(1, ROWS // 8):
                        part = part + sq[8 * i : 8 * i + 8]
                    squares[b, t] += part
                return carry

            lax.fori_loop(0, blocks // UNROLL, step, jnp.zeros((ROWS, LANES), jnp.float32))

    def send_parts(b):
        sums[b] = jnp.sum(squares[b], axis=1, keepdims=True)
        parts[b, mine] = sums[b, my_seq]

        @pl.loop(1, devices)
        def _(d):
            ps, pc, _ = peer(d)
            pltpu.make_async_remote_copy(
                src_ref=sums.at[b, ps], dst_ref=parts.at[b, mine],
                send_sem=part_send.at[b, d], recv_sem=part_recv.at[b, mine],
                device_id=(ps, pc), device_id_type=MESH,
            ).start()

    def seq_peer(d):
        return lax.rem(my_seq + d, seq_size)

    def send_scales(b):
        @pl.loop(1, devices)
        def _(d):
            ps, pc, other = peer(d)
            pltpu.make_async_remote_copy(
                src_ref=sums.at[b, ps], dst_ref=parts.at[b, other],
                send_sem=part_send.at[b, d], recv_sem=part_recv.at[b, other],
                device_id=(ps, pc), device_id_type=MESH,
            ).wait()

        total = jnp.sum(parts[b], axis=0)
        scales[b, my_seq] = lax.rsqrt(total / jnp.float32(width * devices) + 1e-05)

        @pl.loop(1, seq_size)
        def _(d):
            pltpu.make_async_remote_copy(
                src_ref=scales.at[b, my_seq], dst_ref=scales.at[b, my_seq],
                send_sem=scale_send.at[b, d], recv_sem=scale_recv.at[b, my_seq],
                device_id=(seq_peer(d), my_chan), device_id_type=MESH,
            ).start()

    my_rows = pl.ds(pl.multiple_of(my_seq * width, width), width)

    def normalize(b, s):
        send_v[b, s] = (gated[b, s] * scales[b, s] * gain_ref[...]).astype(jnp.bfloat16)

    def data_copy(b, s, d, source):
        return pltpu.make_async_remote_copy(
            src_ref=send_v.at[b, s],
            dst_ref=out_ref.at[b, pl.ds(pl.multiple_of(source * width, width), width), :],
            send_sem=data_send.at[b, d], recv_sem=data_recv.at[b, source],
            device_id=(s, my_chan), device_id_type=MESH,
        )

    def own_copy(b):
        return pltpu.make_async_copy(send_v.at[b, my_seq], out_ref.at[b, my_rows, :], own_sem.at[b])

    def send_data(b):
        @pl.loop(1, seq_size)
        def _(i):
            d = lax.rem(i + seq_size // 2 - 1, seq_size - 1) + 1
            s = seq_peer(d)
            pltpu.make_async_remote_copy(
                src_ref=scales.at[b, s], dst_ref=scales.at[b, s],
                send_sem=scale_send.at[b, d], recv_sem=scale_recv.at[b, s],
                device_id=(s, my_chan), device_id_type=MESH,
            ).wait()
            normalize(b, s)
            data_copy(b, s, d, my_seq).start()

        normalize(b, my_seq)
        own_copy(b).start()

    def finish_data(b):
        @pl.loop(1, seq_size)
        def _(d):
            s = seq_peer(d)
            data_copy(b, s, d, s).wait()

        own_copy(b).wait()

    groups = width // ROWS
    for b in range(batch):
        for copy in loads[b]:
            copy.wait()
        prepare(b)
        if b == 0:
            compute(b, 0, groups)
            pl.semaphore_wait(barrier, devices - 1)
        else:
            compute(b, 0, groups // 2)
            send_scales(b - 1)
            compute(b, groups // 2, groups)
        send_parts(b)
    for b in range(batch - 1):
        send_data(b)
    send_scales(batch - 1)
    send_data(batch - 1)
    for b in range(batch):
        finish_data(b)


def fused(seq_size, chan_size, step_size, inputs, gate_input, decay_rate, norm_gain, resets):
    batch, width, length = step_size.shape
    blocks, devices = length // LANES, seq_size * chan_size
    start = lax.axis_index("seq") * width
    rate, gain = (
        jnp.broadcast_to(lax.dynamic_slice_in_dim(a, start, width)[:, None], (width, LANES))
        for a in (decay_rate, norm_gain)
    )
    f32, dma = jnp.float32, pltpu.SemaphoreType.DMA
    hbm = pl.BlockSpec(memory_space=pl.ANY)
    vmem = pl.BlockSpec(memory_space=pltpu.VMEM)
    return pl.pallas_call(
        functools.partial(kernel, seq_size, chan_size),
        out_shape=jax.ShapeDtypeStruct((batch, width * seq_size, LANES), jnp.bfloat16),
        in_specs=[pl.BlockSpec(memory_space=pltpu.SMEM), hbm, hbm, hbm, vmem, vmem],
        out_specs=hbm,
        scratch_shapes=[
            *(pltpu.VMEM((batch, width, length), jnp.bfloat16) for _ in range(3)),
            pltpu.VMEM((batch, blocks, width, LANES), f32),
            pltpu.VMEM((batch, blocks, width, LANES), jnp.bfloat16),
            pltpu.VMEM((blocks, 8, LANES), f32),
            pltpu.VMEM((batch, blocks, 8, LANES), f32),
            pltpu.VMEM((batch, blocks, 1, LANES), f32),
            pltpu.VMEM((batch, devices, 1, LANES), f32),
            pltpu.VMEM((batch, blocks, 1, LANES), f32),
            dma((batch, 3)),
            dma((batch, devices)), dma((batch, devices)),
            dma((batch, seq_size)), dma((batch, seq_size)),
            dma((batch, seq_size)), dma((batch, seq_size)),
            dma((batch,)),
        ],
        compiler_params=pltpu.CompilerParams(collective_id=0, has_side_effects=True),
    )(resets, step_size, inputs, gate_input, rate, gain)


def solution(mesh):
    seq_size, chan_size = mesh.shape["seq"], mesh.shape["chan"]

    def body(step_size, inputs, gate_input, decay_rate, norm_gain, resets):
        batch, width, length = step_size.shape
        fits = width % ROWS == 0 and length == LANES * seq_size
        if not fits:
            return per_device(step_size, inputs, gate_input, decay_rate, norm_gain, resets)
        return fused(seq_size, chan_size, step_size, inputs, gate_input, decay_rate, norm_gain, resets)

    in_specs = (
        P(None, ("chan", "seq"), None),
        P(None, ("chan", "seq"), None),
        P(None, ("chan", "seq"), None),
        P("chan"),
        P("chan"),
        P(),
    )
    out_specs = P(None, "chan", "seq")
    return jax.shard_map(
        body, mesh=mesh, in_specs=in_specs, out_specs=out_specs, check_vma=False
    )
```

```python
import functools
import math

import jax
import jax.numpy as jnp
from jax import lax
from jax.experimental import pallas as pl
from jax.experimental.pallas import tpu as pltpu
from jax.sharding import PartitionSpec as P

FEATURE_WIDTH = 5120


def compose(earlier, later):
    return (earlier[0] * later[0], later[0] * earlier[1] + later[1])


def coefficients(steps, values, rates):
    scaled = steps.astype(jnp.float32) * rates[None, :, None]
    drive = jnp.sqrt(-jnp.expm1(-2.0 * scaled)) * values.astype(jnp.float32)
    return (scaled, drive)


def marks_for(resets, places):
    return jnp.any(resets[:, :, None] == places[None, None, :], axis=1)


def local_scan(scaled, drive, marks):
    rows, chans, length = scaled.shape
    places = jnp.arange(length, dtype=jnp.int32)
    upper = (places[:, None] <= places[None, :]).astype(jnp.float32)
    cumul = jnp.einsum("rck,ku->rcu", scaled, upper, precision=lax.Precision.HIGHEST)
    counts = jnp.dot(marks.astype(jnp.float32), upper, precision=lax.Precision.HIGHEST)
    linked = (counts[:, :, None] == counts[:, None, :]) & (places[:, None] >= places[None, :])[None]
    group = math.gcd(chans, 64)

    def one_group(pieces):
        cumul_part, drive_part = pieces
        spread = cumul_part[:, :, :, None] - cumul_part[:, :, None, :]
        weight = jnp.where(linked[:, None], jnp.exp(-jnp.maximum(spread, 0.0)), jnp.float32(0.0))
        return jnp.einsum("rctj,rcj->rct", weight, drive_part, precision=lax.Precision.HIGHEST)

    def split_groups(array):
        return jnp.moveaxis(array.reshape(rows, chans // group, group, length), 1, 0)

    results = lax.map(one_group, (split_groups(cumul), split_groups(drive)))
    local_state = jnp.moveaxis(results, 0, 1).reshape(rows, chans, length)
    running = jnp.where(counts[:, None, :] == 0.0, jnp.exp(-cumul), jnp.float32(0.0))
    return (running, local_state)


def finish(gated, norm_gain):
    squares = jnp.sum(gated * gated, axis=1)
    total = lax.psum(squares, "chan")
    mean_square = total / jnp.float32(FEATURE_WIDTH)
    scale_rows = lax.rsqrt(mean_square + 1e-05)
    return (gated * scale_rows[:, None, :] * norm_gain[None, :, None]).astype(jnp.bfloat16)


def per_device(step_size, inputs, gate_input, decay_rate, norm_gain, resets):
    position = lax.axis_index("seq")
    batch, width, length = step_size.shape
    rates = lax.dynamic_slice_in_dim(decay_rate, position * width, width)
    places = jnp.arange(length, dtype=jnp.int32)
    scaled, drive = coefficients(step_size, inputs, rates)
    marks = marks_for(resets, places)
    piece = math.gcd(length, 128)
    count_blocks = length // piece

    def to_blocks(array):
        moved = jnp.moveaxis(array.reshape(batch, width, count_blocks, piece), 2, 1)
        return moved.reshape(batch * count_blocks, width, piece)

    running, local_state = local_scan(
        to_blocks(scaled), to_blocks(drive), marks.reshape(batch * count_blocks, piece)
    )
    total_decay = running[:, :, -1].reshape(batch, count_blocks, width)
    total_state = local_state[:, :, -1].reshape(batch, count_blocks, width)
    prefix = lax.associative_scan(compose, (total_decay, total_state), axis=1)
    incoming = jnp.concatenate(
        [jnp.zeros((batch, 1, width), jnp.float32), prefix[1][:, :-1]], axis=1
    )
    blocked = local_state + running * incoming.reshape(batch * count_blocks, width)[:, :, None]
    state = jnp.moveaxis(blocked.reshape(batch, count_blocks, width, piece), 1, 2).reshape(
        batch, width, length
    )
    local_gated = state * jax.nn.silu(gate_input.astype(jnp.float32))
    gated = lax.all_to_all(local_gated, "seq", split_axis=2, concat_axis=1, tiled=True)
    return finish(gated, norm_gain)


LANES = 128
ROWS = 32
UNROLL = 16
MESH = pl.DeviceIdType.MESH


def scan_blocks(pairs, lane):
    shift = 1
    while shift < LANES:
        inside = lane >= shift
        advanced = []
        for decay, drive in pairs:
            masked = jnp.where(inside, decay, 0.0)
            drive = drive + masked * pltpu.roll(drive, shift, 1)
            decay = jnp.where(inside, decay * pltpu.roll(decay, shift, 1), decay)
            advanced.append((decay, drive))
        pairs = advanced
        shift *= 2
    return pairs


def kernel(
    seq_size, chan_size, resets_ref, step_ref, in_ref, gate_ref, rate_ref, gain_ref, out_ref,
    step_v, in_v, gate_v, gated, send_v, keep, squares, sums, parts, scales,
    load_sem, part_send, part_recv, scale_send, scale_recv, data_send, data_recv, own_sem,
):
    batch, width, length = step_v.shape
    blocks = length // LANES
    devices = seq_size * chan_size
    my_seq, my_chan = lax.axis_index("seq"), lax.axis_index("chan")
    mine = my_seq * chan_size + my_chan

    loads = []
    for b in range(batch):
        group = []
        for i, (src, dst) in enumerate(((step_ref, step_v), (in_ref, in_v), (gate_ref, gate_v))):
            group.append(pltpu.make_async_copy(src.at[b], dst.at[b], load_sem.at[b, i]))
        for copy in group:
            copy.start()
        loads.append(group)

    def peer(d):
        other = lax.rem(mine + d, devices)
        return other // chan_size, lax.rem(other, chan_size), other

    barrier = pltpu.get_barrier_semaphore()

    @pl.loop(1, devices)
    def _(d):
        ps, pc, _ = peer(d)
        pl.semaphore_signal(barrier, inc=1, device_id=(ps, pc), device_id_type=MESH)

    lane = lax.broadcasted_iota(jnp.int32, (ROWS, LANES), 1)
    lane_row = lax.broadcasted_iota(jnp.int32, (8, LANES), 1)
    zero_rows = jnp.zeros((8, LANES), jnp.float32)

    def prepare(b):
        @pl.loop(0, blocks)
        def _(t):
            place = lane_row + t * LANES
            hit = place == resets_ref[b, 0]
            for k in range(1, resets_ref.shape[1]):
                hit = hit | (place == resets_ref[b, k])
            keep[t] = jnp.where(hit, 0.0, 1.0)
            squares[b, t] = zero_rows

    def compute(b, first, last):
        @pl.loop(first, last)
        def _(r):
            rows = pl.ds(pl.multiple_of(r * ROWS, ROWS), ROWS)
            rate = rate_ref[rows, :]

            def step(sup, carry):
                pairs, silus = [], []
                for u in range(UNROLL):
                    t = sup * UNROLL + u
                    lanes = pl.ds(pl.multiple_of(t * LANES, LANES), LANES)
                    x = step_v[b, rows, lanes].astype(jnp.float32) * rate
                    a = jnp.exp(-x)
                    y = x + x
                    series = y * (1.0 - y * (1 / 2 - y * (1 / 6 - y * (1 / 24 - y * (1 / 120 - y * (1 / 720))))))
                    z = jnp.where(y < 0.25, series, 1.0 - a * a)
                    root = z * lax.rsqrt(jnp.maximum(z, 1e-37))
                    drive = root * in_v[b, rows, lanes].astype(jnp.float32)
                    k8 = keep[t]
                    decay = a * jnp.concatenate([k8] * (ROWS // 8), axis=0)
                    pairs.append((decay, drive))
                pairs = scan_blocks(pairs, lane)
                lasts = [
                    [jnp.broadcast_to(a[:, LANES - 1 :], (ROWS, LANES)) for a in pair] for pair in pairs
                ]
                for u in range(UNROLL):
                    t = sup * UNROLL + u
                    lanes = pl.ds(pl.multiple_of(t * LANES, LANES), LANES)
                    decay, drive = pairs[u]
                    state = drive + decay * carry
                    carry = lasts[u][1] + lasts[u][0] * carry
                    v = gate_v[b, rows, lanes].astype(jnp.float32)
                    g = state * (v / (1.0 + jnp.exp(-v)))
                    gated[b, t, rows, :] = g
                    sq = g * g
                    part = sq[:8]
                    for i in range(1, ROWS // 8):
                        part = part + sq[8 * i : 8 * i + 8]
                    squares[b, t] += part
                return carry

            lax.fori_loop(0, blocks // UNROLL, step, jnp.zeros((ROWS, LANES), jnp.float32))

    def send_parts(b):
        sums[b] = jnp.sum(squares[b], axis=1, keepdims=True)
        parts[b, mine] = sums[b, my_seq]

        @pl.loop(1, devices)
        def _(d):
            ps, pc, _ = peer(d)
            pltpu.make_async_remote_copy(
                src_ref=sums.at[b, ps], dst_ref=parts.at[b, mine],
                send_sem=part_send.at[b, d], recv_sem=part_recv.at[b, mine],
                device_id=(ps, pc), device_id_type=MESH,
            ).start()

    def seq_peer(d):
        return lax.rem(my_seq + d, seq_size)

    def send_scales(b):
        @pl.loop(1, devices)
        def _(d):
            ps, pc, other = peer(d)
            pltpu.make_async_remote_copy(
                src_ref=sums.at[b, ps], dst_ref=parts.at[b, other],
                send_sem=part_send.at[b, d], recv_sem=part_recv.at[b, other],
                device_id=(ps, pc), device_id_type=MESH,
            ).wait()

        total = jnp.sum(parts[b], axis=0)
        scales[b, my_seq] = lax.rsqrt(total / jnp.float32(width * devices) + 1e-05)

        @pl.loop(1, seq_size)
        def _(d):
            pltpu.make_async_remote_copy(
                src_ref=scales.at[b, my_seq], dst_ref=scales.at[b, my_seq],
                send_sem=scale_send.at[b, d], recv_sem=scale_recv.at[b, my_seq],
                device_id=(seq_peer(d), my_chan), device_id_type=MESH,
            ).start()

    my_rows = pl.ds(pl.multiple_of(my_seq * width, width), width)

    def normalize(b, s):
        send_v[b, s] = (gated[b, s] * scales[b, s] * gain_ref[...]).astype(jnp.bfloat16)

    def data_copy(b, s, d, source):
        return pltpu.make_async_remote_copy(
            src_ref=send_v.at[b, s],
            dst_ref=out_ref.at[b, pl.ds(pl.multiple_of(source * width, width), width), :],
            send_sem=data_send.at[b, d], recv_sem=data_recv.at[b, source],
            device_id=(s, my_chan), device_id_type=MESH,
        )

    def own_copy(b):
        return pltpu.make_async_copy(send_v.at[b, my_seq], out_ref.at[b, my_rows, :], own_sem.at[b])

    def send_data(b):
        @pl.loop(1, seq_size)
        def _(i):
            d = lax.rem(i + seq_size // 2 - 1, seq_size - 1) + 1
            s = seq_peer(d)
            pltpu.make_async_remote_copy(
                src_ref=scales.at[b, s], dst_ref=scales.at[b, s],
                send_sem=scale_send.at[b, d], recv_sem=scale_recv.at[b, s],
                device_id=(s, my_chan), device_id_type=MESH,
            ).wait()
            normalize(b, s)
            data_copy(b, s, d, my_seq).start()

        normalize(b, my_seq)
        own_copy(b).start()

    def finish_data(b):
        @pl.loop(1, seq_size)
        def _(d):
            s = seq_peer(d)
            data_copy(b, s, d, s).wait()

        own_copy(b).wait()

    groups = width // ROWS
    for b in range(batch):
        for copy in loads[b]:
            copy.wait()
        prepare(b)
        if b == 0:
            compute(b, 0, groups)
            pl.semaphore_wait(barrier, devices - 1)
        else:
            compute(b, 0, groups // 2)
            send_scales(b - 1)
            compute(b, groups // 2, groups)
        send_parts(b)
    for b in range(batch - 1):
        send_data(b)
    send_scales(batch - 1)
    send_data(batch - 1)
    for b in range(batch):
        finish_data(b)


def fused(seq_size, chan_size, step_size, inputs, gate_input, decay_rate, norm_gain, resets):
    batch, width, length = step_size.shape
    blocks, devices = length // LANES, seq_size * chan_size
    start = lax.axis_index("seq") * width
    rate, gain = (
        jnp.broadcast_to(lax.dynamic_slice_in_dim(a, start, width)[:, None], (width, LANES))
        for a in (decay_rate, norm_gain)
    )
    f32, dma = jnp.float32, pltpu.SemaphoreType.DMA
    hbm = pl.BlockSpec(memory_space=pl.ANY)
    vmem = pl.BlockSpec(memory_space=pltpu.VMEM)
    return pl.pallas_call(
        functools.partial(kernel, seq_size, chan_size),
        out_shape=jax.ShapeDtypeStruct((batch, width * seq_size, LANES), jnp.bfloat16),
        in_specs=[pl.BlockSpec(memory_space=pltpu.SMEM), hbm, hbm, hbm, vmem, vmem],
        out_specs=hbm,
        scratch_shapes=[
            *(pltpu.VMEM((batch, width, length), jnp.bfloat16) for _ in range(3)),
            pltpu.VMEM((batch, blocks, width, LANES), f32),
            pltpu.VMEM((batch, blocks, width, LANES), jnp.bfloat16),
            pltpu.VMEM((blocks, 8, LANES), f32),
            pltpu.VMEM((batch, blocks, 8, LANES), f32),
            pltpu.VMEM((batch, blocks, 1, LANES), f32),
            pltpu.VMEM((batch, devices, 1, LANES), f32),
            pltpu.VMEM((batch, blocks, 1, LANES), f32),
            dma((batch, 3)),
            dma((batch, devices)), dma((batch, devices)),
            dma((batch, seq_size)), dma((batch, seq_size)),
            dma((batch, seq_size)), dma((batch, seq_size)),
            dma((batch,)),
        ],
        compiler_params=pltpu.CompilerParams(collective_id=0, has_side_effects=True),
    )(resets, step_size, inputs, gate_input, rate, gain)


def solution(mesh):
    seq_size, chan_size = mesh.shape["seq"], mesh.shape["chan"]

    def body(step_size, inputs, gate_input, decay_rate, norm_gain, resets):
        batch, width, length = step_size.shape
        fits = width % ROWS == 0 and length == LANES * seq_size
        if not fits:
            return per_device(step_size, inputs, gate_input, decay_rate, norm_gain, resets)
        return fused(seq_size, chan_size, step_size, inputs, gate_input, decay_rate, norm_gain, resets)

    in_specs = (
        P(None, ("chan", "seq"), None),
        P(None, ("chan", "seq"), None),
        P(None, ("chan", "seq"), None),
        P("chan"),
        P("chan"),
        P(),
    )
    out_specs = P(None, "chan", "seq")
    return jax.shard_map(
        body, mesh=mesh, in_specs=in_specs, out_specs=out_specs, check_vma=False
    )
```

```python
import functools
import math

import jax
import jax.numpy as jnp
from jax import lax
from jax.experimental import pallas as pl
from jax.experimental.pallas import tpu as pltpu
from jax.sharding import PartitionSpec as P

FEATURE_WIDTH = 5120


def compose(earlier, later):
    return (earlier[0] * later[0], later[0] * earlier[1] + later[1])


def coefficients(steps, values, rates):
    scaled = steps.astype(jnp.float32) * rates[None, :, None]
    drive = jnp.sqrt(-jnp.expm1(-2.0 * scaled)) * values.astype(jnp.float32)
    return (scaled, drive)


def marks_for(resets, places):
    return jnp.any(resets[:, :, None] == places[None, None, :], axis=1)


def local_scan(scaled, drive, marks):
    rows, chans, length = scaled.shape
    places = jnp.arange(length, dtype=jnp.int32)
    upper = (places[:, None] <= places[None, :]).astype(jnp.float32)
    cumul = jnp.einsum("rck,ku->rcu", scaled, upper, precision=lax.Precision.HIGHEST)
    counts = jnp.dot(marks.astype(jnp.float32), upper, precision=lax.Precision.HIGHEST)
    linked = (counts[:, :, None] == counts[:, None, :]) & (places[:, None] >= places[None, :])[None]
    group = math.gcd(chans, 64)

    def one_group(pieces):
        cumul_part, drive_part = pieces
        spread = cumul_part[:, :, :, None] - cumul_part[:, :, None, :]
        weight = jnp.where(linked[:, None], jnp.exp(-jnp.maximum(spread, 0.0)), jnp.float32(0.0))
        return jnp.einsum("rctj,rcj->rct", weight, drive_part, precision=lax.Precision.HIGHEST)

    def split_groups(array):
        return jnp.moveaxis(array.reshape(rows, chans // group, group, length), 1, 0)

    results = lax.map(one_group, (split_groups(cumul), split_groups(drive)))
    local_state = jnp.moveaxis(results, 0, 1).reshape(rows, chans, length)
    running = jnp.where(counts[:, None, :] == 0.0, jnp.exp(-cumul), jnp.float32(0.0))
    return (running, local_state)


def finish(gated, norm_gain):
    squares = jnp.sum(gated * gated, axis=1)
    total = lax.psum(squares, "chan")
    mean_square = total / jnp.float32(FEATURE_WIDTH)
    scale_rows = lax.rsqrt(mean_square + 1e-05)
    return (gated * scale_rows[:, None, :] * norm_gain[None, :, None]).astype(jnp.bfloat16)


def per_device(step_size, inputs, gate_input, decay_rate, norm_gain, resets):
    position = lax.axis_index("seq")
    batch, width, length = step_size.shape
    rates = lax.dynamic_slice_in_dim(decay_rate, position * width, width)
    places = jnp.arange(length, dtype=jnp.int32)
    scaled, drive = coefficients(step_size, inputs, rates)
    marks = marks_for(resets, places)
    piece = math.gcd(length, 128)
    count_blocks = length // piece

    def to_blocks(array):
        moved = jnp.moveaxis(array.reshape(batch, width, count_blocks, piece), 2, 1)
        return moved.reshape(batch * count_blocks, width, piece)

    running, local_state = local_scan(
        to_blocks(scaled), to_blocks(drive), marks.reshape(batch * count_blocks, piece)
    )
    total_decay = running[:, :, -1].reshape(batch, count_blocks, width)
    total_state = local_state[:, :, -1].reshape(batch, count_blocks, width)
    prefix = lax.associative_scan(compose, (total_decay, total_state), axis=1)
    incoming = jnp.concatenate(
        [jnp.zeros((batch, 1, width), jnp.float32), prefix[1][:, :-1]], axis=1
    )
    blocked = local_state + running * incoming.reshape(batch * count_blocks, width)[:, :, None]
    state = jnp.moveaxis(blocked.reshape(batch, count_blocks, width, piece), 1, 2).reshape(
        batch, width, length
    )
    local_gated = state * jax.nn.silu(gate_input.astype(jnp.float32))
    gated = lax.all_to_all(local_gated, "seq", split_axis=2, concat_axis=1, tiled=True)
    return finish(gated, norm_gain)


LANES = 128
ROWS = 32
INNER = 4
UNROLL = 16
MESH = pl.DeviceIdType.MESH


def scan_blocks(pairs, lane):
    shift = 1
    while shift < LANES:
        inside = lane >= shift
        advanced = []
        for decay, drive in pairs:
            masked = jnp.where(inside, decay, 0.0)
            drive = drive + masked * pltpu.roll(drive, shift, 1)
            decay = jnp.where(inside, decay * pltpu.roll(decay, shift, 1), decay)
            advanced.append((decay, drive))
        pairs = advanced
        shift *= 2
    return pairs


def kernel(
    seq_size, chan_size, resets_ref, step_ref, in_ref, gate_ref, rate_ref, gain_ref, out_ref,
    step_v, in_v, gate_v, small_v, columns, gated, send_v, keep, squares, near, far, scales,
    load_sem, small_sem, near_send, near_recv, far_send, far_recv, data_send, data_recv, own_sem,
):
    batch, width, length = step_v.shape
    blocks = length // LANES
    devices = seq_size * chan_size
    my_seq, my_chan = lax.axis_index("seq"), lax.axis_index("chan")
    mine = my_seq * chan_size + my_chan
    inner = math.gcd(seq_size, INNER)
    outer = seq_size // inner
    plane = inner * chan_size
    my_place, my_outer = lax.rem(mine, plane), mine // plane

    smalls = [
        pltpu.make_async_copy(src, small_v.at[i], small_sem.at[i]) for i, src in enumerate((rate_ref, gain_ref))
    ]
    for copy in smalls:
        copy.start()
    loads = []
    for b in range(batch):
        group = []
        for i, (src, dst) in enumerate(((step_ref, step_v), (in_ref, in_v), (gate_ref, gate_v))):
            group.append(pltpu.make_async_copy(src.at[b], dst.at[b], load_sem.at[b, i]))
        for copy in group:
            copy.start()
        loads.append(group)

    def peer(d):
        other = lax.rem(mine + d, devices)
        return other // chan_size, lax.rem(other, chan_size), other

    barrier = pltpu.get_barrier_semaphore()

    @pl.loop(1, devices)
    def _(d):
        ps, pc, _ = peer(d)
        pl.semaphore_signal(barrier, inc=1, device_id=(ps, pc), device_id_type=MESH)

    lane = lax.broadcasted_iota(jnp.int32, (ROWS, LANES), 1)
    lane_row = lax.broadcasted_iota(jnp.int32, (8, LANES), 1)
    zero_rows = jnp.zeros((8, LANES), jnp.float32)

    def prepare(b):
        @pl.loop(0, blocks)
        def _(t):
            place = lane_row + t * LANES
            hit = place == resets_ref[b, 0]
            for n in range(1, resets_ref.shape[1]):
                hit = hit | (place == resets_ref[b, n])
            keep[b, t] = jnp.where(hit, 0.0, 1.0)
            squares[b, t] = zero_rows

    first_channel = my_seq * width
    channel_row, channel_shift = first_channel // LANES, lax.rem(first_channel, LANES)

    def make_columns():
        for i in range(2):
            for n in range(columns.shape[1] // LANES):
                row = small_v[i, pl.ds(jnp.minimum(channel_row + n, small_v.shape[1] - 1), 1), :]
                columns[i, n * LANES : (n + 1) * LANES, :] = jnp.transpose(jnp.broadcast_to(row, (LANES, LANES)))

    def column(i, start, size):
        return columns[i, pl.ds(pl.multiple_of(channel_shift + start, math.gcd(width, LANES)), size), :]

    def compute(b, first, last):
        @pl.loop(first, last)
        def _(r):
            rows = pl.ds(pl.multiple_of(r * ROWS, ROWS), ROWS)
            rate = column(0, r * ROWS, ROWS)

            def step(sup, carry):
                pairs, silus = [], []
                for u in range(UNROLL):
                    t = sup * UNROLL + u
                    lanes = pl.ds(pl.multiple_of(t * LANES, LANES), LANES)
                    x = step_v[b, rows, lanes].astype(jnp.float32) * rate
                    a = jnp.exp(-x)
                    y = x + x
                    series = y * (1.0 - y * (1 / 2 - y * (1 / 6 - y * (1 / 24 - y * (1 / 120 - y * (1 / 720))))))
                    z = jnp.where(y < 0.25, series, 1.0 - a * a)
                    root = z * lax.rsqrt(jnp.maximum(z, 1e-37))
                    drive = root * in_v[b, rows, lanes].astype(jnp.float32)
                    k8 = keep[b, t]
                    decay = a * jnp.concatenate([k8] * (ROWS // 8), axis=0)
                    pairs.append((decay, drive))
                pairs = scan_blocks(pairs, lane)
                lasts = [
                    [jnp.broadcast_to(a[:, LANES - 1 :], (ROWS, LANES)) for a in pair] for pair in pairs
                ]
                for u in range(UNROLL):
                    t = sup * UNROLL + u
                    lanes = pl.ds(pl.multiple_of(t * LANES, LANES), LANES)
                    decay, drive = pairs[u]
                    state = drive + decay * carry
                    carry = lasts[u][1] + lasts[u][0] * carry
                    v = gate_v[b, rows, lanes].astype(jnp.float32)
                    g = state * (v / (1.0 + jnp.exp(-v)))
                    gated[b, t, rows, :] = g
                    sq = g * g
                    part = sq[:8]
                    for i in range(1, ROWS // 8):
                        part = part + sq[8 * i : 8 * i + 8]
                    squares[b, t] += part
                return carry

            lax.fori_loop(0, blocks // UNROLL, step, jnp.zeros((ROWS, LANES), jnp.float32))

    def near_copy(b, d, source):
        place = lax.rem(my_place + d, plane)
        return pltpu.make_async_remote_copy(
            src_ref=near.at[b, my_place], dst_ref=near.at[b, source],
            send_sem=near_send.at[b, d], recv_sem=near_recv.at[b, source],
            device_id=(my_outer * inner + place // chan_size, lax.rem(place, chan_size)), device_id_type=MESH,
        )

    def far_copy(b, d, source):
        place = lax.rem(my_outer + d, outer)
        return pltpu.make_async_remote_copy(
            src_ref=far.at[b, my_outer], dst_ref=far.at[b, source],
            send_sem=far_send.at[b, d], recv_sem=far_recv.at[b, source],
            device_id=(place * inner + lax.rem(my_seq, inner), my_chan), device_id_type=MESH,
        )

    def send_near(b):
        near[b, my_place] = jnp.sum(squares[b], axis=1)

        @pl.loop(1, plane)
        def _(d):
            near_copy(b, d, my_place).start()

    def send_far(b):
        @pl.loop(1, plane)
        def _(d):
            near_copy(b, d, lax.rem(my_place + d, plane)).wait()

        far[b, my_outer] = jnp.sum(near[b], axis=0)

        @pl.loop(1, outer)
        def _(d):
            far_copy(b, d, my_outer).start()

    def make_scales(b):
        @pl.loop(1, outer)
        def _(d):
            far_copy(b, d, lax.rem(my_outer + d, outer)).wait()

        total = jnp.sum(far[b], axis=0)
        scales[b] = lax.rsqrt(total / jnp.float32(width * devices) + 1e-05)

    def seq_peer(d):
        return lax.rem(my_seq + d, seq_size)

    my_rows = pl.ds(pl.multiple_of(my_seq * width, width), width)

    def normalize(b, s):
        send_v[b, s] = (gated[b, s] * scales[b, pl.ds(s, 1), :] * column(1, 0, width)).astype(jnp.bfloat16)

    def data_copy(b, s, d, source):
        return pltpu.make_async_remote_copy(
            src_ref=send_v.at[b, s],
            dst_ref=out_ref.at[b, pl.ds(pl.multiple_of(source * width, width), width), :],
            send_sem=data_send.at[b, d], recv_sem=data_recv.at[b, source],
            device_id=(s, my_chan), device_id_type=MESH,
        )

    def own_copy(b):
        return pltpu.make_async_copy(send_v.at[b, my_seq], out_ref.at[b, my_rows, :], own_sem.at[b])

    def send_data(b):
        @pl.loop(1, seq_size)
        def _(d):
            s = seq_peer(d)
            normalize(b, s)
            data_copy(b, s, d, my_seq).start()

        normalize(b, my_seq)
        own_copy(b).start()

    def finish_data(b):
        @pl.loop(1, seq_size)
        def _(d):
            s = seq_peer(d)
            data_copy(b, s, d, s).wait()

        own_copy(b).wait()

    groups = width // ROWS
    for b in range(batch):
        prepare(b)
    for copy in smalls:
        copy.wait()
    make_columns()
    for b in range(batch):
        for copy in loads[b]:
            copy.wait()
        if b == 0:
            compute(b, 0, groups)
            pl.semaphore_wait(barrier, devices - 1)
        else:
            split = groups * 3 // 5
            compute(b, 0, split)
            send_far(b - 1)
            compute(b, split, groups)
        send_near(b)
    for b in range(batch - 1):
        make_scales(b)
        send_data(b)
    send_far(batch - 1)
    make_scales(batch - 1)
    send_data(batch - 1)
    for b in range(batch):
        finish_data(b)


def fused(seq_size, chan_size, step_size, inputs, gate_input, decay_rate, norm_gain, resets):
    batch, width, length = step_size.shape
    blocks, devices = length // LANES, seq_size * chan_size
    inner = math.gcd(seq_size, INNER)
    outer, plane = seq_size // inner, inner * chan_size
    rate, gain = decay_rate.reshape(-1, LANES), norm_gain.reshape(-1, LANES)
    span = LANES - math.gcd(width, LANES) + width
    column_rows = -(-span // LANES) * LANES
    f32, dma = jnp.float32, pltpu.SemaphoreType.DMA
    hbm = pl.BlockSpec(memory_space=pl.ANY)
    return pl.pallas_call(
        functools.partial(kernel, seq_size, chan_size),
        out_shape=jax.ShapeDtypeStruct((batch, width * seq_size, LANES), jnp.bfloat16),
        in_specs=[pl.BlockSpec(memory_space=pltpu.SMEM), hbm, hbm, hbm, hbm, hbm],
        out_specs=hbm,
        scratch_shapes=[
            *(pltpu.VMEM((batch, width, length), jnp.bfloat16) for _ in range(3)),
            pltpu.VMEM((2, *rate.shape), f32),
            pltpu.VMEM((2, column_rows, LANES), f32),
            pltpu.VMEM((batch, blocks, width, LANES), f32),
            pltpu.VMEM((batch, blocks, width, LANES), jnp.bfloat16),
            pltpu.VMEM((batch, blocks, 8, LANES), f32),
            pltpu.VMEM((batch, blocks, 8, LANES), f32),
            pltpu.VMEM((batch, plane, blocks, LANES), f32),
            pltpu.VMEM((batch, outer, blocks, LANES), f32),
            pltpu.VMEM((batch, blocks, LANES), f32),
            dma((batch, 3)), dma((2,)),
            dma((batch, plane)), dma((batch, plane)),
            dma((batch, outer)), dma((batch, outer)),
            dma((batch, seq_size)), dma((batch, seq_size)),
            dma((batch,)),
        ],
        compiler_params=pltpu.CompilerParams(collective_id=0, has_side_effects=True),
    )(resets, step_size, inputs, gate_input, rate, gain)


def solution(mesh):
    seq_size, chan_size = mesh.shape["seq"], mesh.shape["chan"]

    def body(step_size, inputs, gate_input, decay_rate, norm_gain, resets):
        batch, width, length = step_size.shape
        fits = width % ROWS == 0 and length == LANES * seq_size
        fits = fits and (width * seq_size) % LANES == 0
        if not fits:
            return per_device(step_size, inputs, gate_input, decay_rate, norm_gain, resets)
        return fused(seq_size, chan_size, step_size, inputs, gate_input, decay_rate, norm_gain, resets)

    in_specs = (
        P(None, ("chan", "seq"), None),
        P(None, ("chan", "seq"), None),
        P(None, ("chan", "seq"), None),
        P("chan"),
        P("chan"),
        P(),
    )
    out_specs = P(None, "chan", "seq")
    return jax.shard_map(
        body, mesh=mesh, in_specs=in_specs, out_specs=out_specs, check_vma=False
    )
```
